8 devices in a mesh: tp: 4 (over z, y, x), dp: 2 (over core).
Axes of the slice: x: 2, y: 2, z: 1, core: 2. Of those that a mesh axis runs over, the one named last changes fastest.
Arguments:
- x: bfloat16 [4096, 8192], P(('dp', 'tp'))
- w_gate: bfloat16 [8192, 28672], P('dp', 'tp')
- w_up: bfloat16 [8192, 28672], P('dp', 'tp')
- w_down: bfloat16 [28672, 8192], P('tp', 'dp')
Outputs:
- output: bfloat16 [4096, 8192], P(('dp', 'tp'))
All inputs are finite; a program needn't handle non-finite values.
Results may differ from the reference program's by a relative error of at most 0.0131236.
Values are sent between devices in bfloat16 or wider.
A program may use at most 1 GiB of HBM per device.

```python
import jax
import jax.numpy as jnp
from jax import lax

D = 8192
FF = 28672
TOKENS_DEV = 512
ROWS = 4096

NBLK = ROWS // TOKENS_DEV


def setup_inputs(seed: int = 0) -> dict:
    k = jax.random.split(jax.random.key(seed), 4)
    x = jax.random.normal(k[0], (ROWS, D), jnp.float32)
    wg = jax.random.normal(k[1], (D, FF), jnp.float32) * D ** -0.5
    wu = jax.random.normal(k[2], (D, FF), jnp.float32) * D ** -0.5
    wd = jax.random.normal(k[3], (FF, D), jnp.float32) * FF ** -0.5
    return {"x": x.astype(jnp.bfloat16), "w_gate": wg.astype(jnp.bfloat16), "w_up": wu.astype(jnp.bfloat16), "w_down": wd.astype(jnp.bfloat16)}


def reference(x, w_gate, w_up, w_down):
    def blk(xb):
        a = jnp.dot(xb, w_gate, preferred_element_type=jnp.float32)
        b = jnp.dot(xb, w_up, preferred_element_type=jnp.float32)
        h = (jax.nn.silu(a) * b).astype(jnp.bfloat16)
        o = jnp.dot(h, w_down, preferred_element_type=jnp.float32)
        return (xb.astype(jnp.float32) + o).astype(jnp.bfloat16)
    y = lax.map(blk, x.reshape(NBLK, TOKENS_DEV, D))
    return y.reshape(ROWS, D)
```

```python
import functools

import jax
import jax.numpy as jnp
from jax import lax
from jax.experimental import pallas as pl
from jax.experimental.pallas import tpu as pltpu
from jax.sharding import PartitionSpec as P


BF = jnp.bfloat16
F32 = jnp.float32
VMEM_BYTES = 67_000_000


def mm(a, b):
    return jnp.dot(a, b, preferred_element_type=F32)


def first_step(fn):
    pl.when(pl.program_id(0) == 0)(fn)


def up_tiles(base, x, w, xv, wv, xsem, wsem):
    i, n = pl.program_id(0), pl.num_programs(0)
    tn = wv.shape[-1]
    slot = lax.rem(i, 2)

    def w_copy(t, j):
        at, cols = lax.rem(t, 2), pl.ds(pl.multiple_of(base + t * tn, tn), tn)
        return pltpu.make_async_copy(w[j].at[:, cols], wv.at[at, j], wsem.at[at, j])

    def x_copy(c):
        return pltpu.make_async_copy(x[c], xv.at[c], xsem.at[c])

    @first_step
    def _():
        x_copy(0).start()
        w_copy(0, 0).start()

    w_copy(i, 0).wait()

    @first_step
    def _():
        x_copy(0).wait()
        w_copy(0, 1).start()
        x_copy(1).start()

    a = mm(xv[0], wv[slot, 0])
    w_copy(i, 1).wait()

    @pl.when(i + 1 < n)
    def _():
        w_copy(i + 1, 0).start()
        w_copy(i + 1, 1).start()

    yield 0, a, mm(xv[0], wv[slot, 1])

    @first_step
    def _():
        x_copy(1).wait()

    yield 1, mm(xv[1], wv[slot, 0]), mm(xv[1], wv[slot, 1])


def give_kernel(rows, half, start, off, x0, x1, wg, wu, pa, pb, *scratch):
    base = off[0] * half + start
    for c, a, b in up_tiles(base, (x0, x1), (wg, wu), *scratch):
        pa[pl.ds(c * rows, rows), :] = a.astype(BF)
        pb[pl.ds(c * rows, rows), :] = b.astype(BF)


def keep_kernel(rows, half, start, off, x0, x1, wg, wu, ra, rb, h, *scratch):
    base = off[0] * half + start
    for c, a, b in up_tiles(base, (x0, x1), (wg, wu), *scratch):
        theirs = pl.ds((1 - c) * rows, rows)
        a = a + ra[theirs, :].astype(F32)
        b = b + rb[theirs, :].astype(F32)
        h[pl.ds(c * rows, rows), :] = (jax.nn.silu(a) * b).astype(BF)


def down_kernel(rows, half, starts, chunks, n_add, off, *refs):
    n_h = len(starts)
    own, got, wd = refs[:n_h], refs[n_h : 2 * n_h], refs[2 * n_h]
    refs = refs[2 * n_h + 1 :]
    adds, outs = refs[:n_add], refs[n_add : n_add + len(chunks)]
    hv, wv, hsem, wsem = refs[-4:]
    i, n = pl.program_id(0), pl.num_programs(0)
    tn = wv.shape[-1]

    def w_copy(t):
        at, cols = lax.rem(t, 2), pl.ds(pl.multiple_of(t * tn, tn), tn)
        return pltpu.make_async_copy(wd.at[:, cols], wv.at[at], wsem.at[at])

    def h_copies(k):
        for j, start in enumerate(starts):
            for g, (src, c, side) in enumerate(((own[j], chunks[k], off[0]), (got[j], 1 - chunks[k], 1 - off[0]))):
                cols = pl.ds(pl.multiple_of(side * half + start, 128), src.shape[1])
                yield pltpu.make_async_copy(
                    src.at[pl.ds(c * rows, rows), :], hv.at[k, :, cols], hsem.at[k, j, g]
                )

    @first_step
    def _():
        for c in h_copies(0):
            c.start()
        w_copy(0).start()

    w_copy(i).wait()

    @first_step
    def _():
        for c in h_copies(0):
            c.wait()
        if len(chunks) > 1:
            for c in h_copies(1):
                c.start()

    @pl.when(i + 1 < n)
    def _():
        w_copy(i + 1).start()

    for k in range(len(chunks)):
        if k:

            @first_step
            def _():
                for c in h_copies(k):
                    c.wait()

        o = mm(hv[k], wv[lax.rem(i, 2)])
        if n_add:
            o = o + adds[k][...].astype(F32)
        outs[k][...] = o.astype(BF)


def finish_kernel(off, x, m0, m1, p0, p1, y):
    n = m0.shape[1]
    for at, lhs, rhs in ((off[0], m0, m1), (1 - off[0], p0, p1)):
        cols = pl.ds(pl.multiple_of(at * n, 128), n)
        o = lhs[...].astype(F32) + rhs[...].astype(F32)
        y[:, cols] = (x[:, cols].astype(F32) + o).astype(BF)


def solution(mesh):
    nt = mesh.shape["tp"]
    nd = mesh.shape["dp"]
    axes = ("tp", "dp")

    def pairs(bit0, bit1, flip):
        return [(t * nd + d, (t ^ (bit0, bit1)[d]) * nd + (d ^ flip)) for t in range(nt) for d in range(nd)]

    perms = {"a": pairs(1, 2, 0), "b": pairs(2, 1, 0), "c": pairs(0, 0, 1), "ax": pairs(1, 2, 1), "bx": pairs(2, 1, 1)}

    def body(x, wg, wu, wd):
        r, d = x.shape
        dc = d // nd
        f = wg.shape[1]
        half, tn = f // 2, 512
        tiles = half // tn
        cut = (tiles + 1) // 2
        whole, parts = ((0, tiles),), ((0, cut), (cut, tiles - cut))
        me = lax.axis_index("dp")
        mine, other = me.reshape(1), (1 - me).reshape(1)
        last = [None]
        anywhere = pl.BlockSpec(memory_space=pl.ANY)
        params = pltpu.CompilerParams(dimension_semantics=("arbitrary",), vmem_limit_bytes=VMEM_BYTES)

        def hop(v, kind):
            return lax.ppermute(v, axes, perms[kind])

        def after(v):
            if last[0] is None:
                return v
            return lax.optimization_barrier((v, last[0]))[0]

        def run(call, args):
            out = call(*args)
            last[0] = out[0] if isinstance(out, (list, tuple)) else out
            return out

        def up(kernel, who, span, xs, extra, n_out):
            start, count = span
            t_spec = pl.BlockSpec((2 * r, tn), lambda i, o: (0, i))
            width = count * tn
            call = pl.pallas_call(
                functools.partial(kernel, r, half, start * tn),
                grid_spec=pltpu.PrefetchScalarGridSpec(
                    num_scalar_prefetch=1,
                    grid=(count,),
                    in_specs=[anywhere] * 4 + [t_spec] * len(extra),
                    out_specs=[t_spec] * n_out,
                    scratch_shapes=[
                        pltpu.VMEM((2, r, dc), BF),
                        pltpu.VMEM((2, 2, dc, tn), BF),
                        pltpu.SemaphoreType.DMA((2,)),
                        pltpu.SemaphoreType.DMA((2, 2)),
                    ],
                ),
                out_shape=[jax.ShapeDtypeStruct((2 * r, width), BF)] * n_out,
                compiler_params=params,
                cost_estimate=pl.CostEstimate(
                    flops=8 * r * dc * width, bytes_accessed=4 * (r * dc + dc * width + r * width), transcendentals=0
                ),
            )
            return run(call, (who, after(xs[0]), xs[1], wg, wu, *extra))

        def give(xs, spans=whole, q=0):
            pa, pb = up(give_kernel, other, spans[q], xs, (), 2)
            return hop(pa, "c"), hop(pb, "c")

        def keep(xs, got, spans=whole, q=0):
            (h,) = up(keep_kernel, mine, spans[q], xs, got, 1)
            return h, hop(h, "c"), spans[q][0] * tn

        def down(hs, chunks, adds=()):
            own, got, starts = zip(*hs)
            n = len(chunks)
            o_spec = pl.BlockSpec((r, tn), lambda i, o: (0, i))
            call = pl.pallas_call(
                functools.partial(down_kernel, r, half, starts, chunks, len(adds)),
                grid_spec=pltpu.PrefetchScalarGridSpec(
                    num_scalar_prefetch=1,
                    grid=(dc // tn,),
                    in_specs=[anywhere] * (2 * len(hs) + 1) + [o_spec] * len(adds),
                    out_specs=[o_spec] * n,
                    scratch_shapes=[
                        pltpu.VMEM((n, r, f), BF),
                        pltpu.VMEM((2, f, tn), BF),
                        pltpu.SemaphoreType.DMA((n, len(hs), 2)),
                        pltpu.SemaphoreType.DMA((2,)),
                    ],
                ),
                out_shape=[jax.ShapeDtypeStruct((r, dc), BF)] * n,
                compiler_params=params,
                cost_estimate=pl.CostEstimate(
                    flops=2 * n * r * f * dc, bytes_accessed=2 * (n * r * f + f * dc + n * r * dc), transcendentals=0
                ),
            )
            return run(call, (mine, after(own[0]), *own[1:], *got, wd, *adds))

        xm = lax.dynamic_slice_in_dim(x, me * dc, dc, 1)
        xp = hop(lax.dynamic_slice_in_dim(x, (1 - me) * dc, dc, 1), "c")
        x1m = hop(xm, "a")
        x1p = hop(xp, "b")
        u0 = (xm, xp)
        g00 = give(u0, parts, 0)
        g01 = give(u0, parts, 1)
        k00 = keep(u0, g00, parts, 0)
        x2m, x2p = hop(x1m, "b"), hop(x1p, "a")
        k01 = keep(u0, g01, parts, 1)
        u1, u2 = (x1m, x1p), (x2m, x2p)
        g1 = give(u1)
        x3m, x3p = hop(xm, "b"), hop(xp, "a")
        u3 = (x3m, x3p)
        g2 = give(u2)
        k1 = keep(u1, g1)
        k2 = keep(u2, g2)
        g3 = give(u3)
        o2m, o2p = down((k2,), (0, 1))
        s2m, s2p = hop(o2m, "a"), hop(o2p, "b")
        o1m, o1p = down((k1,), (0, 1))
        y1m, y1p = hop(o1m, "a"), hop(o1p, "b")
        k3 = keep(u3, g3)
        (o3p,) = down((k3,), (1,), (s2p,))
        y3p = hop(o3p, "ax")
        (o3m,) = down((k3,), (0,), (s2m,))
        y3m = hop(o3m, "b")
        (op,) = down((k00, k01), (1,), (y1p,))
        rp = hop(op, "c")
        (om,) = down((k00, k01), (0,), (y1m,))
        rows = min(r, 64)
        half = pl.BlockSpec((rows, dc), lambda i, o: (i, 0))
        full = pl.BlockSpec((rows, d), lambda i, o: (i, 0))
        call = pl.pallas_call(
            finish_kernel,
            grid_spec=pltpu.PrefetchScalarGridSpec(
                num_scalar_prefetch=1, grid=(r // rows,), in_specs=[full] + [half] * 4, out_specs=full
            ),
            out_shape=jax.ShapeDtypeStruct((r, d), BF),
            compiler_params=pltpu.CompilerParams(dimension_semantics=("arbitrary",)),
            cost_estimate=pl.CostEstimate(flops=3 * r * d, bytes_accessed=8 * r * d, transcendentals=0),
            name="finish",
        )
        return run(call, (mine, x, om, y3m, rp, y3p))

    return jax.shard_map(body, mesh=mesh, in_specs=(P(("dp", "tp"), None), P("dp", "tp"), P("dp", "tp"), P("tp", "dp")), out_specs=P(("dp", "tp"), None), check_vma=False)
```

```python
import functools

import jax
import jax.numpy as jnp
from jax import lax
from jax.experimental import pallas as pl
from jax.experimental.pallas import tpu as pltpu
from jax.sharding import PartitionSpec as P


BF = jnp.bfloat16
F32 = jnp.float32
VMEM_BYTES = 67_000_000


def mm(a, b):
    return jnp.dot(a, b, preferred_element_type=F32)


def first_step(fn):
    pl.when(pl.program_id(0) == 0)(fn)


def up_tiles(base, x, w, got, xv, wv, xsem, wsem, rv=None, rsem=None):
    i, n = pl.program_id(0), pl.num_programs(0)
    tn = wv.shape[-1]
    slot = lax.rem(i, 2)

    def w_copy(t, j):
        at, cols = lax.rem(t, 2), pl.ds(pl.multiple_of(base + t * tn, tn), tn)
        return pltpu.make_async_copy(w[j].at[:, cols], wv.at[at, j], wsem.at[at, j])

    def r_copy(t, j):
        at, cols = lax.rem(t, 2), pl.ds(pl.multiple_of(t * tn, tn), tn)
        return pltpu.make_async_copy(got[j].at[:, cols], rv.at[at, j], rsem.at[at, j])

    def x_copy(c):
        return pltpu.make_async_copy(x[c], xv.at[c], xsem.at[c])

    @first_step
    def _():
        x_copy(0).start()
        w_copy(0, 0).start()

    w_copy(i, 0).wait()

    @first_step
    def _():
        x_copy(0).wait()
        w_copy(0, 1).start()
        for c in range(1, len(x)):
            x_copy(c).start()
        for j in range(len(got)):
            r_copy(0, j).start()

    first = mm(xv[0], wv[slot, 0])
    w_copy(i, 1).wait()

    @first_step
    def _():
        for c in range(1, len(x)):
            x_copy(c).wait()

    for j in range(len(got)):
        r_copy(i, j).wait()

    @pl.when(i + 1 < n)
    def _():
        for j in range(2):
            w_copy(i + 1, j).start()
        for j in range(len(got)):
            r_copy(i + 1, j).start()

    out = [(first, mm(xv[0], wv[slot, 1]))]
    for c in range(1, len(x)):
        out.append((mm(xv[c], wv[slot, 0]), mm(xv[c], wv[slot, 1])))
    return out


def give_kernel(rows, half, chunks, off, *refs):
    x, (wg, wu, pa, pb), scratch = refs[:chunks], refs[chunks : chunks + 4], refs[chunks + 4 :]
    for c, (a, b) in enumerate(up_tiles(off[0] * half, x, (wg, wu), (), *scratch)):
        pa[pl.ds(c * rows, rows), :] = a.astype(BF)
        pb[pl.ds(c * rows, rows), :] = b.astype(BF)


def keep_kernel(rows, half, chunks, off, *refs):
    x, (wg, wu, ra, rb, h), scratch = refs[:chunks], refs[chunks : chunks + 5], refs[chunks + 5 :]
    rv = scratch[4]
    slot = lax.rem(pl.program_id(0), 2)
    for c, (a, b) in enumerate(up_tiles(off[0] * half, x, (wg, wu), (ra, rb), *scratch)):
        theirs = pl.ds((chunks - 1 - c) * rows, rows)
        a = a + rv[slot, 0, theirs, :].astype(F32)
        b = b + rv[slot, 1, theirs, :].astype(F32)
        h[pl.ds(c * rows, rows), :] = (jax.nn.silu(a) * b).astype(BF)


def down_kernel(rows, half, chunks, n_add, off, own, got, wd, *refs):
    adds, outs = refs[:n_add], refs[n_add : n_add + len(chunks)]
    hv, wv, hsem, wsem = refs[-4:]
    i, n = pl.program_id(0), pl.num_programs(0)
    tn = wv.shape[-1]

    def w_copy(t):
        at, cols = lax.rem(t, 2), pl.ds(pl.multiple_of(t * tn, tn), tn)
        return pltpu.make_async_copy(wd.at[:, cols], wv.at[at], wsem.at[at])

    def h_copies(k):
        for g, (src, c, side) in enumerate(((own, chunks[k][0], off[0]), (got, chunks[k][1], 1 - off[0]))):
            cols = pl.ds(pl.multiple_of(side * half, 128), half)
            yield pltpu.make_async_copy(src.at[pl.ds(c * rows, rows), :], hv.at[k, :, cols], hsem.at[k, g])

    @first_step
    def _():
        for c in h_copies(0):
            c.start()
        w_copy(0).start()

    w_copy(i).wait()

    @first_step
    def _():
        for c in h_copies(0):
            c.wait()
        if len(chunks) > 1:
            for c in h_copies(1):
                c.start()

    @pl.when(i + 1 < n)
    def _():
        w_copy(i + 1).start()

    for k in range(len(chunks)):
        if k:

            @first_step
            def _():
                for c in h_copies(k):
                    c.wait()

        o = mm(hv[k], wv[lax.rem(i, 2)])
        if n_add:
            o = o + adds[k][...].astype(F32)
        outs[k][...] = o.astype(BF)


def finish_kernel(off, x, m0, m1, p0, p1, y):
    n = m0.shape[1]
    for at, lhs, rhs in ((off[0], m0, m1), (1 - off[0], p0, p1)):
        cols = pl.ds(pl.multiple_of(at * n, 128), n)
        o = lhs[...].astype(F32) + rhs[...].astype(F32)
        y[:, cols] = (x[:, cols].astype(F32) + o).astype(BF)


def solution(mesh):
    nt = mesh.shape["tp"]
    nd = mesh.shape["dp"]
    axes = ("tp", "dp")

    def pairs(bit0, bit1, flip):
        return [(t * nd + d, (t ^ (bit0, bit1)[d]) * nd + (d ^ flip)) for t in range(nt) for d in range(nd)]

    perms = {"a": pairs(1, 2, 0), "b": pairs(2, 1, 0), "c": pairs(0, 0, 1), "ax": pairs(1, 2, 1), "bx": pairs(2, 1, 1)}

    def body(x, wg, wu, wd):
        r, d = x.shape
        dc = d // nd
        f = wg.shape[1]
        half, tn = f // 2, 512
        me = lax.axis_index("dp")
        mine, other = me.reshape(1), (1 - me).reshape(1)
        last = [None]
        anywhere = pl.BlockSpec(memory_space=pl.ANY)
        params = pltpu.CompilerParams(dimension_semantics=("arbitrary",), vmem_limit_bytes=VMEM_BYTES)

        def hop(v, kind):
            return lax.ppermute(v, axes, perms[kind])

        def after(v):
            if last[0] is None:
                return v
            return lax.optimization_barrier((v, last[0]))[0]

        def run(call, args):
            out = call(*args)
            last[0] = out[0] if isinstance(out, (list, tuple)) else out
            return out

        def up(kernel, who, xs, got, n_out):
            n = len(xs)
            shape = jax.ShapeDtypeStruct((n * r, half), BF)
            scratch = [
                pltpu.VMEM((n, r, dc), BF),
                pltpu.VMEM((2, 2, dc, tn), BF),
                pltpu.SemaphoreType.DMA((n,)),
                pltpu.SemaphoreType.DMA((2, 2)),
            ]
            if got:
                scratch += [pltpu.VMEM((2, 2, n * r, tn), BF), pltpu.SemaphoreType.DMA((2, 2))]
            call = pl.pallas_call(
                functools.partial(kernel, r, half, n),
                grid_spec=pltpu.PrefetchScalarGridSpec(
                    num_scalar_prefetch=1,
                    grid=(half // tn,),
                    in_specs=[anywhere] * (n + 2 + len(got)),
                    out_specs=[pl.BlockSpec((n * r, tn), lambda i, o: (0, i))] * n_out,
                    scratch_shapes=scratch,
                ),
                out_shape=[shape] * n_out,
                compiler_params=params,
                cost_estimate=pl.CostEstimate(
                    flops=4 * n * r * dc * half, bytes_accessed=4 * (n * r + half) * dc, transcendentals=0
                ),
            )
            return run(call, (who, after(xs[0]), *xs[1:], wg, wu, *got))

        def give(xs):
            pa, pb = up(give_kernel, other, xs, (), 2)
            return hop(pa, "c"), hop(pb, "c")

        def keep(xs, got):
            (h,) = up(keep_kernel, mine, xs, got, 1)
            return h, hop(h, "c")

        def down(own, got, chunks, adds=()):
            n = len(chunks)
            o_spec = pl.BlockSpec((r, tn), lambda i, o: (0, i))
            call = pl.pallas_call(
                functools.partial(down_kernel, r, half, chunks, len(adds)),
                grid_spec=pltpu.PrefetchScalarGridSpec(
                    num_scalar_prefetch=1,
                    grid=(dc // tn,),
                    in_specs=[anywhere] * 3 + [o_spec] * len(adds),
                    out_specs=[o_spec] * n,
                    scratch_shapes=[
                        pltpu.VMEM((n, r, f), BF),
                        pltpu.VMEM((2, f, tn), BF),
                        pltpu.SemaphoreType.DMA((n, 2)),
                        pltpu.SemaphoreType.DMA((2,)),
                    ],
                ),
                out_shape=[jax.ShapeDtypeStruct((r, dc), BF)] * n,
                compiler_params=params,
                cost_estimate=pl.CostEstimate(
                    flops=2 * n * r * f * dc, bytes_accessed=2 * (n * r * f + f * dc + n * r * dc), transcendentals=0
                ),
            )
            return run(call, (mine, after(own), got, wd, *adds))

        xm = lax.dynamic_slice_in_dim(x, me * dc, dc, 1)
        xp = hop(lax.dynamic_slice_in_dim(x, (1 - me) * dc, dc, 1), "c")
        x1m = hop(xm, "a")
        g0m = give((xm,))
        x1p = hop(xp, "b")
        g0p = give((xp,))
        x2m = hop(x1m, "b")
        h0p, t0p = keep((xp,), g0m)
        x2p = hop(x1p, "a")
        u1, u2 = (x1m, x1p), (x2m, x2p)
        g1 = give(u1)
        x3m, x3p = hop(xm, "b"), hop(xp, "a")
        u3 = (x3m, x3p)
        g2 = give(u2)
        h1, t1 = keep(u1, g1)
        h2, t2 = keep(u2, g2)
        g3 = give(u3)
        both = ((0, 1), (1, 0))
        o2m, o2p = down(h2, t2, both)
        s2m, s2p = hop(o2m, "a"), hop(o2p, "b")
        o1m, o1p = down(h1, t1, both)
        y1m, y1p = hop(o1m, "a"), hop(o1p, "b")
        h3, t3 = keep(u3, g3)
        h0m, t0m = keep((xm,), g0p)
        (o3p,) = down(h3, t3, both[1:], (s2p,))
        y3p = hop(o3p, "ax")
        (o3m,) = down(h3, t3, both[:1], (s2m,))
        y3m = hop(o3m, "b")
        (op,) = down(h0p, t0m, ((0, 0),), (y1p,))
        rp = hop(op, "c")
        (om,) = down(h0m, t0p, ((0, 0),), (y1m,))
        rows = min(r, 64)
        half = pl.BlockSpec((rows, dc), lambda i, o: (i, 0))
        full = pl.BlockSpec((rows, d), lambda i, o: (i, 0))
        call = pl.pallas_call(
            finish_kernel,
            grid_spec=pltpu.PrefetchScalarGridSpec(
                num_scalar_prefetch=1, grid=(r // rows,), in_specs=[full] + [half] * 4, out_specs=full
            ),
            out_shape=jax.ShapeDtypeStruct((r, d), BF),
            compiler_params=pltpu.CompilerParams(dimension_semantics=("arbitrary",)),
            cost_estimate=pl.CostEstimate(flops=3 * r * d, bytes_accessed=8 * r * d, transcendentals=0),
            name="finish",
        )
        return run(call, (mine, x, om, y3m, rp, y3p))

    return jax.shard_map(body, mesh=mesh, in_specs=(P(("dp", "tp"), None), P("dp", "tp"), P("dp", "tp"), P("tp", "dp")), out_specs=P(("dp", "tp"), None), check_vma=False)
```
